32 devices in a mesh: mem: 8 (over y, x, core), pix: 4 (over z).
Axes of the slice: x: 2, y: 2, z: 4, core: 2. Of those that a mesh axis runs over, the one named last changes fastest.
Arguments:
- prior_motion: bfloat16 [64, 16, 131072], P('mem', None, 'pix'), may hold values from -6 to 6
- measured_motion: float32 [1200], replicated, may hold values from -1.6 to 1.6
- measurement_noise_stddev: float32 [1200], replicated, may hold values from 0.05 to 0.5
- gaussian_jitter: float32 [2, 1200, 64], replicated, may hold values from -6 to 6
- scene_couples: int32 [2, 1200], replicated, may hold values from 0 to 15, as said below
- targeted_tile_number: int32 [1200], replicated, may hold values from 0 to 2047
Outputs:
- analysis: bfloat16 [64, 16, 131072], P('mem', None, 'pix')
The draws below stay inside these ranges and needn't reach their ends.
Inputs may be any that keep to these rules, and one draw needn't show every extreme that they name: scene_couples[0, k] < scene_couples[1, k]: row 0 holds the earlier acquisition, row 1 the later.
All inputs are finite; a program needn't handle non-finite values.
Results may differ from the reference program's by a relative error of at most 0.011.
Values may be sent and summed in bfloat16 or wider, within the bound.
A program may use at most 192 MiB of HBM per device.

```python
import math
import jax
import jax.numpy as jnp
from jax import lax

REALIZATION_NUM = 64
SCENE_TIMES = 16
NOBS = 1200
BLK = 64
PASS_COUNT = 2
RASTER_CELLS = 131072
NBLK = 2048
N_MEM = 8
N_PIX = 4


def draw_scene_couples(key, part):
    key_first = jax.random.fold_in(key, 11)
    key_gap = jax.random.fold_in(key, 12)
    earlier = jax.random.randint(key_first, (NOBS,), 0, SCENE_TIMES - 1)
    offset = jax.random.randint(key_gap, (NOBS,), 0, SCENE_TIMES - 1)
    later = earlier + 1 + offset % (SCENE_TIMES - 1 - earlier)
    return jnp.stack([earlier, later]).astype(jnp.int32)


def plant(entries, rng, least, largest):
    extent = entries.shape
    index_at = [jax.random.randint(jax.random.fold_in(rng, axis), (), 0, extent[axis]) for axis in range(len(extent))]
    entries = entries.at[tuple(index_at)].set(least)
    longest = extent.index(max(extent))
    index_at[longest] = (index_at[longest] + 1) % extent[longest]
    return entries.at[tuple(index_at)].set(largest)


def level_of(key, extent, split, low, top_value):
    factor_of, own = 1.0, jax.random.fold_in(key, 6)
    for position, blocks in split:
        draws = jnp.exp(jax.random.uniform(jax.random.fold_in(own, position), (blocks,), jnp.float32, low / len(split), top_value / len(split)))
        factor_of = factor_of * jnp.repeat(draws, extent[position] // blocks).reshape([-1 if axis == position else 1 for axis in range(len(extent))])
    return factor_of


def noise(key, shape, width, most, split=(), kind=jnp.bfloat16):
    entries = jax.random.normal(key, shape, jnp.float32) * width
    if len(split) > 0:
        entries = level_of(key, shape, split, -0.22, 0.18) * entries
    return jnp.clip(entries, min=-most, max=most).astype(kind)


def setup_inputs(seed: int = 0) -> dict:
    arg_keys = jax.random.split(jax.random.key(seed), 7)
    prior_motion = noise(arg_keys[0], (REALIZATION_NUM, SCENE_TIMES, RASTER_CELLS), 1.0, 6.0, ((0, 8), (2, 4)))
    measured_motion = noise(arg_keys[1], (NOBS,), 0.2, 1.6, (), jnp.float32)
    measurement_noise_stddev = jnp.clip(jnp.exp(jax.random.uniform(arg_keys[2], (NOBS,), jnp.float32, math.log(0.05), math.log(0.5))), 0.05, 0.5)
    gaussian_jitter = noise(arg_keys[3], (PASS_COUNT, NOBS, REALIZATION_NUM), 1.0, 6.0, (), jnp.float32)
    scene_couples = draw_scene_couples(jax.random.fold_in(arg_keys[6], 71), 0)
    targeted_tile_number = plant(jax.random.randint(arg_keys[5], (NOBS,), 0, NBLK), jax.random.fold_in(arg_keys[5], 1), 0, NBLK - 1).astype(jnp.int32)
    return {"prior_motion": prior_motion, "measured_motion": measured_motion, "measurement_noise_stddev": measurement_noise_stddev, "gaussian_jitter": gaussian_jitter, "scene_couples": scene_couples, "targeted_tile_number": targeted_tile_number}


def update_tile(tile_state, mixing):
    realization_vectors = tile_state.shape[0]
    average = lax.optimization_barrier(jnp.sum(tile_state, axis=0, dtype=jnp.float32)) / realization_vectors
    anomaly = (tile_state.astype(jnp.float32) - average).astype(jnp.bfloat16)
    change = jnp.dot(mixing.T.astype(jnp.float32), anomaly.reshape(realization_vectors, -1).astype(jnp.float32), preferred_element_type=jnp.float32)
    return (tile_state.astype(jnp.float32) + change.reshape(tile_state.shape)).astype(jnp.bfloat16)

def reference(prior_motion, measured_motion, measurement_noise_stddev, gaussian_jitter, scene_couples, targeted_tile_number):
    realization_vectors = prior_motion.shape[0]
    spread_factor = float(PASS_COUNT)
    member_anomaly = jnp.sqrt(jnp.float32(spread_factor)) * measurement_noise_stddev
    ground_motion_vector = prior_motion
    for iteration in range(PASS_COUNT):
        sums = lax.optimization_barrier(jnp.sum(ground_motion_vector.reshape(realization_vectors, SCENE_TIMES, NBLK, BLK), axis=3, dtype=jnp.float32))
        predicted = ((sums[:, scene_couples[1], targeted_tile_number] - sums[:, scene_couples[0], targeted_tile_number]) / BLK).T
        centred = predicted - lax.optimization_barrier(jnp.mean(predicted, axis=1, keepdims=True))
        scaled = centred / (member_anomaly[:, None] * math.sqrt(realization_vectors - 1))
        misfit = (measured_motion[:, None] + member_anomaly[:, None] * gaussian_jitter[iteration] - predicted) / member_anomaly[:, None]
        gram = jnp.dot(scaled.T.astype(jnp.float32), scaled.astype(jnp.float32), precision=lax.Precision.HIGHEST, preferred_element_type=jnp.float32)
        cross = jnp.dot(scaled.T.astype(jnp.float32), misfit.astype(jnp.float32), precision=lax.Precision.HIGHEST, preferred_element_type=jnp.float32)
        factor = jnp.linalg.cholesky(jnp.eye(realization_vectors, dtype=jnp.float32) + gram)
        mixing = (jax.scipy.linalg.cho_solve((factor, True), cross) / math.sqrt(realization_vectors - 1)).astype(jnp.bfloat16)
        tiles = jnp.moveaxis(ground_motion_vector.reshape(realization_vectors, SCENE_TIMES, N_PIX * N_MEM, -1), 2, 0)

        def one_tile(tile_state):
            return update_tile(tile_state, mixing)
        fresh = lax.map(one_tile, tiles)
        ground_motion_vector = jnp.moveaxis(fresh, 0, 2).reshape(ground_motion_vector.shape)
    return ground_motion_vector
```

```python
import functools
import math

import jax
import jax.numpy as jnp
from jax import lax
from jax.experimental import pallas as pl
from jax.experimental.pallas import tpu as pltpu
from jax.sharding import PartitionSpec as P

BLK = 64
PASS_COUNT = 2
F32 = jnp.float32
BF16 = jnp.bfloat16
HI = lax.Precision.HIGHEST


def nn(a, b):
    return lax.dot_general(a, b, (((1,), (0,)), ((), ())), precision=HI, preferred_element_type=F32)


def tn(a, b):
    return nn(a.T, b)


def nt(a, b):
    return lax.dot_general(a, b, (((1,), (1,)), ((), ())), precision=HI, preferred_element_type=F32)


def iota(shape, axis):
    return lax.broadcasted_iota(jnp.int32, shape, axis)


def observe_kernel(times, x_ref, target_ref, couples_ref, out_ref, acc):
    step = pl.program_id(0)
    rows, width = x_ref.shape
    blocks = width // BLK
    obs = target_ref.shape[1]
    summer = (iota((width, blocks), 0) // BLK == iota((width, blocks), 1)).astype(BF16)
    sums = jnp.dot(x_ref[...], summer, preferred_element_type=F32)
    table = (target_ref[...] - step * blocks == iota((blocks, obs), 0)).astype(F32)
    part = nn(sums, table)

    @pl.when(step == 0)
    def _():
        acc[...] = part

    @pl.when(step > 0)
    def _():
        acc[...] += part

    @pl.when(step == pl.num_programs(0) - 1)
    def _():
        scene = iota((rows, obs), 0) % times
        pair = (scene == couples_ref[1:2, :]).astype(F32) - (scene == couples_ref[0:1, :]).astype(F32)
        members = out_ref.shape[0]
        group = (iota((members, rows), 1) // times == iota((members, rows), 0)).astype(F32)
        out_ref[...] = nn(group, acc[...] * pair) / BLK


def observe(x, target, couples):
    members, times, cells = x.shape
    obs = target.shape[1]
    width = math.gcd(cells, 4096)
    rows = members * times
    return pl.pallas_call(
        functools.partial(observe_kernel, times),
        grid=(cells // width,),
        in_specs=[
            pl.BlockSpec((rows, width), lambda i: (0, i)),
            pl.BlockSpec((1, obs), lambda i: (0, 0)),
            pl.BlockSpec((2, obs), lambda i: (0, 0)),
        ],
        out_specs=pl.BlockSpec((members, obs), lambda i: (0, 0)),
        out_shape=jax.ShapeDtypeStruct((members, obs), F32),
        scratch_shapes=[pltpu.VMEM((rows, obs), F32)],
        name="observe",
    )(x.reshape(rows, cells), target, couples)


def stats_kernel(tile_blocks, pred_ref, target_ref, measured_ref, noise_ref, jitter_ref, out_ref):
    pred = pred_ref[...]
    target = target_ref[...]
    here = ((target >= 0) & (target < tile_blocks)).astype(F32)
    mean = jnp.mean(pred, axis=0, keepdims=True)
    scale = math.sqrt(float(PASS_COUNT)) * noise_ref[...]
    centred = (pred - mean) / scale * here
    gap = jnp.broadcast_to((measured_ref[...] - mean) / scale * here, pred.shape)
    right = jnp.concatenate([centred, gap, jitter_ref[0], jitter_ref[1]], axis=0)
    out_ref[...] = nt(centred, right)


def gauss_jordan(matrix, right):
    n = matrix.shape[0]
    work = jnp.concatenate([matrix, right], axis=1)
    row_id = iota((n, 1), 0)
    for k in range(n):
        pivot = work[k : k + 1, :] / work[k : k + 1, k : k + 1]
        factor = jnp.where(row_id == k, 0.0, work[:, k : k + 1])
        work = jnp.where(row_id == k, pivot, work - factor * pivot)
    return work[:, n:]


def mix_kernel(times, me_ref, stats_ref, out_ref):
    total = stats_ref[0]
    for i in range(1, stats_ref.shape[0]):
        total = total + stats_ref[i]
    n = total.shape[0]
    s, g, h1, h2 = (total[:, i * n : (i + 1) * n] for i in range(4))
    eye = (iota((n, n), 0) == iota((n, n), 1)).astype(F32)
    m1 = gauss_jordan(eye + s / (n - 1), (g + h1 - s) / (n - 1)).astype(BF16).astype(F32)
    m1_mean = jnp.mean(m1, axis=1, keepdims=True)
    step = eye + m1 - m1_mean
    s2 = tn(step, nn(s, step))
    g2 = tn(step, g - nn(s, jnp.broadcast_to(m1_mean, (n, n))))
    h22 = tn(step, h2)
    m2 = gauss_jordan(eye + s2 / (n - 1), (g2 + h22 - s2) / (n - 1)).astype(BF16).astype(F32)
    m2c = m2 - jnp.mean(m2, axis=0, keepdims=True)
    w = m1 + m2 + nn(m1, m2c)
    w = w - jnp.mean(w, axis=0, keepdims=True)

    parts, two_rows, depth = out_ref.shape
    rows = two_rows // 2
    members = n // parts
    spot = iota((n, n), 0)
    source = ((spot // members) ^ me_ref[0]) * members + spot % members
    order = (iota((n, n), 1) == source).astype(F32)
    wt = nt(nn(order, w.T), order)
    hi = wt.astype(BF16)
    lo = (wt - hi.astype(F32)).astype(BF16)
    spread = (iota((n, depth), 1) // times == iota((n, depth), 0)).astype(BF16)
    tall = (iota((rows, members), 0) // times == iota((rows, members), 1)).astype(BF16)
    same = iota((rows, depth), 0) % times == iota((rows, depth), 1) % times
    for piece, first in ((hi, 0), (lo, rows)):
        wide = jnp.dot(piece, spread, preferred_element_type=F32).astype(BF16)
        for part in range(parts):
            block = jnp.dot(
                tall, wide[part * members : (part + 1) * members, :], preferred_element_type=F32
            )
            out_ref[part, first : first + rows, :] = jnp.where(same, block, 0.0).astype(BF16)


def update_kernel(which, mix_ref, *refs):
    out_ref = refs[-1]
    rows = out_ref.shape[0]
    state = jnp.concatenate([ref[...] for ref in refs[:-1]], axis=0)
    both = jnp.dot(mix_ref[0], state, preferred_element_type=F32)
    out_ref[...] = (refs[which][...].astype(F32) + both[:rows] + both[rows:]).astype(BF16)


def update(which, mix, pieces):
    rows, width = pieces[0].shape
    tile = math.gcd(width, 1024)
    spec = pl.BlockSpec((rows, tile), lambda i: (0, i))
    return pl.pallas_call(
        functools.partial(update_kernel, which),
        grid=(width // tile,),
        in_specs=[pl.BlockSpec((1,) + mix.shape[1:], lambda i: (which, 0, 0))] + [spec] * len(pieces),
        out_specs=spec,
        out_shape=jax.ShapeDtypeStruct((rows, width), BF16),
        name=f"update{which}",
    )(mix, *pieces)


def body(prior, measured, noise, jitter, couples, target):
    parts = lax.axis_size("mem")
    me = lax.axis_index("mem")
    members, times, cells = prior.shape
    total_members = members * parts
    width = cells // parts
    tile_blocks = cells // BLK
    obs = target.shape[0]
    extra = (-obs) % 128

    def padded(a, value):
        return jnp.pad(a, [(0, 0)] * (a.ndim - 1) + [(0, extra)], constant_values=value)

    target_row = padded(target[None, :] - lax.axis_index("pix") * tile_blocks, -1)
    couple_rows = padded(couples, 0)
    measured_row = padded(measured[None, :], 0.0)
    noise_row = padded(noise[None, :], 1.0)
    jitter_rows = padded(jnp.swapaxes(jitter, 1, 2), 0.0)

    predicted = observe(prior, target_row, couple_rows)
    predicted = lax.all_gather(predicted, "mem", axis=0, tiled=True)
    prior, predicted = lax.optimization_barrier((prior, predicted))

    flat = prior.reshape(members * times, cells)

    def perm(k):
        return [(i, i ^ k) for i in range(parts)]

    def part_of(k):
        return lax.dynamic_slice_in_dim(flat, (me ^ k) * width, width, axis=1)

    pieces = [part_of(0)] + [None] * (parts - 1)
    for k in reversed(range(1, parts)):
        pieces[k] = lax.ppermute(part_of(k), "mem", perm(k))

    stats = pl.pallas_call(
        functools.partial(stats_kernel, tile_blocks),
        out_shape=jax.ShapeDtypeStruct((total_members, 4 * total_members), F32),
        name="stats",
    )(predicted, target_row, measured_row, noise_row, jitter_rows)
    stats = lax.all_gather(stats, "pix", axis=0, tiled=False)
    rows = members * times
    mix = pl.pallas_call(
        functools.partial(mix_kernel, times),
        in_specs=[
            pl.BlockSpec(memory_space=pltpu.SMEM),
            pl.BlockSpec(memory_space=pltpu.VMEM),
        ],
        out_shape=jax.ShapeDtypeStruct((parts, 2 * rows, rows * parts), BF16),
        name="mix",
    )(me.astype(jnp.int32).reshape(1), stats)

    out = jnp.zeros((rows, cells), BF16)
    moved = [None] * parts
    for k in reversed(range(parts)):
        fresh = update(k, mix, pieces)
        moved[k] = lax.ppermute(fresh, "mem", perm(k)) if k else fresh
    for k in reversed(range(parts)):
        out = lax.dynamic_update_slice_in_dim(out, moved[k], (me ^ k) * width, axis=1)
    return out.reshape(prior.shape)


def solution(mesh):
    return jax.shard_map(
        body,
        mesh=mesh,
        in_specs=(P("mem", None, "pix"), P(), P(), P(), P(), P()),
        out_specs=P("mem", None, "pix"),
        check_vma=False,
    )
```

```python
import functools
import math

import jax
import jax.numpy as jnp
from jax import lax
from jax.experimental import pallas as pl
from jax.experimental.pallas import tpu as pltpu
from jax.sharding import PartitionSpec as P

BLK = 64
PASS_COUNT = 2
F32 = jnp.float32
BF16 = jnp.bfloat16
HI = lax.Precision.HIGHEST


def nn(a, b):
    return lax.dot_general(a, b, (((1,), (0,)), ((), ())), precision=HI, preferred_element_type=F32)


def tn(a, b):
    return nn(a.T, b)


def nt(a, b):
    return lax.dot_general(a, b, (((1,), (1,)), ((), ())), precision=HI, preferred_element_type=F32)


def iota(shape, axis):
    return lax.broadcasted_iota(jnp.int32, shape, axis)


def gauss_jordan(matrix, right):
    n = matrix.shape[0]
    work = jnp.concatenate([matrix, right], axis=1)
    row_id = iota((n, 1), 0)
    for k in range(n):
        pivot = work[k : k + 1, :] / work[k : k + 1, k : k + 1]
        factor = jnp.where(row_id == k, 0.0, work[:, k : k + 1])
        work = jnp.where(row_id == k, pivot, work - factor * pivot)
    return work[:, n:]


HALVES = 2


def flip(me, k, parts):
    total, bit = 0, 1
    while bit < parts:
        total = total + bit * ((me // bit + k // bit) % 2)
        bit *= 2
    return total


def fold(total):
    n = total.shape[0]
    s, g, h1, h2 = (total[:, i * n : (i + 1) * n] for i in range(4))
    eye = (iota((n, n), 0) == iota((n, n), 1)).astype(F32)
    m1 = gauss_jordan(eye + s / (n - 1), (g + h1 - s) / (n - 1)).astype(BF16).astype(F32)
    m1_mean = jnp.mean(m1, axis=1, keepdims=True)
    step = eye + m1 - m1_mean
    s2 = tn(step, nn(s, step))
    g2 = tn(step, g - nn(s, jnp.broadcast_to(m1_mean, (n, n))))
    h22 = tn(step, h2)
    m2 = gauss_jordan(eye + s2 / (n - 1), (g2 + h22 - s2) / (n - 1)).astype(BF16).astype(F32)
    m2c = m2 - jnp.mean(m2, axis=0, keepdims=True)
    w = m1 + m2 + nn(m1, m2c)
    return w - jnp.mean(w, axis=0, keepdims=True)


def expand(w, me, parts, times, mix):
    n = w.shape[0]
    members = n // parts
    rows = members * times
    depth = rows * parts
    spot = iota((n, n), 0)
    source = flip(me, spot // members, parts) * members + spot % members
    order = (iota((n, n), 1) == source).astype(F32)
    wt = nt(nn(order, w.T), order)
    hi = wt.astype(BF16)
    lo = (wt - hi.astype(F32)).astype(BF16)
    spread = (iota((n, depth), 1) // times == iota((n, depth), 0)).astype(BF16)
    tall = (iota((rows, members), 0) // times == iota((rows, members), 1)).astype(BF16)
    same = iota((rows, depth), 0) % times == iota((rows, depth), 1) % times
    for piece, first in ((hi, 0), (lo, rows)):
        wide = jnp.dot(piece, spread, preferred_element_type=F32).astype(BF16)
        for part in range(parts):
            block = jnp.dot(
                tall, wide[part * members : (part + 1) * members, :], preferred_element_type=F32
            )
            mix[part, first : first + rows, :] = jnp.where(same, block, 0.0).astype(BF16)


def smoother_kernel(
    parts, tiles, times,
    x, measured, noise, jitter, couples, target, out,
    held, fresh, mix, window, acc, pred, stats, tgt, pairs, meas, sigma, draws,
    in_send, in_recv, out_send, out_recv, pred_send, pred_recv, stat_send, stat_recv,
    window_sem, own_sem,
):
    me, tile = lax.axis_index("mem"), lax.axis_index("pix")
    rows, cells = x.shape
    members = rows // times
    width = cells // parts
    half = width // HALVES
    tile_blocks = cells // BLK
    obs = target.shape[1]
    peers = [flip(me, k, parts) for k in range(parts)]
    order = list(range(2, parts, 2)) + list(range(3, parts, 2)) + [1]

    barrier = pltpu.get_barrier_semaphore()
    for k in range(1, parts):
        pl.semaphore_signal(barrier, inc=1, device_id={"mem": peers[k], "pix": tile}, device_id_type=pl.DeviceIdType.MESH)
    for q in range(1, tiles):
        pl.semaphore_signal(barrier, inc=1, device_id={"mem": me, "pix": flip(tile, q, tiles)}, device_id_type=pl.DeviceIdType.MESH)
    pl.semaphore_wait(barrier, parts + tiles - 2)

    def columns(part, h):
        return pl.ds(pl.multiple_of(part * width + h * half, 128), half)

    def inward(k, h):
        return pltpu.make_async_remote_copy(
            src_ref=x.at[:, columns(peers[k], h)],
            dst_ref=held.at[pl.ds(k * rows, rows), pl.ds(h * half, half)],
            send_sem=in_send.at[k, h], recv_sem=in_recv.at[k, h],
            device_id={"mem": peers[k], "pix": tile}, device_id_type=pl.DeviceIdType.MESH,
        )

    def outward(k, h):
        return pltpu.make_async_remote_copy(
            src_ref=fresh.at[k, :, pl.ds(h * half, half)],
            dst_ref=out.at[:, columns(me, h)],
            send_sem=out_send.at[k, h], recv_sem=out_recv.at[k, h],
            device_id={"mem": peers[k], "pix": tile}, device_id_type=pl.DeviceIdType.MESH,
        )

    early = order[: (parts - 1) // 2]
    for k in early:
        inward(k, 0).start()
    own_in = [pltpu.make_async_copy(x.at[:, columns(me, h)], held.at[pl.ds(0, rows), pl.ds(h * half, half)], in_recv.at[0, h]) for h in range(HALVES)]

    span = window.shape[2]
    blocks = span // BLK
    steps = cells // span
    wide = acc.shape[1]

    def fetch(i):
        slot = i % 2
        return pltpu.make_async_copy(x.at[:, pl.ds(pl.multiple_of(i * span, 128), span)], window.at[slot], window_sem.at[slot])

    fetch(0).start()
    tgt[...] = jnp.full(tgt.shape, -1, jnp.int32)
    tgt[:, :obs] = target[...] - tile * tile_blocks
    pairs[...] = jnp.zeros_like(pairs)
    pairs[:, :obs] = couples[...]
    meas[...] = jnp.zeros_like(meas)
    meas[:, :obs] = measured[...]
    sigma[...] = jnp.ones_like(sigma)
    sigma[:, :obs] = noise[...]
    draws[...] = jnp.zeros_like(draws)
    draws[:, :, :obs] = jitter[...]
    acc[...] = jnp.zeros_like(acc)
    summer = (iota((span, blocks), 0) // BLK == iota((span, blocks), 1)).astype(BF16)
    targets = tgt[...]
    block_id = iota((blocks, wide), 0)

    for i in range(steps):
        if i + 1 < steps:
            fetch(i + 1).start()
        fetch(i).wait()
        sums = jnp.dot(window[i % 2], summer, preferred_element_type=F32)
        table = (targets - i * blocks == block_id).astype(F32).astype(BF16)
        rest = sums
        part = None
        for _ in range(3):
            piece = rest.astype(BF16)
            rest = rest - piece.astype(F32)
            term = jnp.dot(piece, table, preferred_element_type=F32)
            part = term if part is None else part + term
        acc[...] += part
    scene = iota((rows, wide), 0) % times
    pair = (scene == pairs[1:2, :]).astype(F32) - (scene == pairs[0:1, :]).astype(F32)
    group = (iota((members, rows), 1) // times == iota((members, rows), 0)).astype(F32)
    pred[0] = nn(group, acc[...] * pair) / BLK

    def tell(k):
        return pltpu.make_async_remote_copy(
            src_ref=pred.at[0], dst_ref=pred.at[k],
            send_sem=pred_send.at[k], recv_sem=pred_recv.at[k],
            device_id={"mem": peers[k], "pix": tile}, device_id_type=pl.DeviceIdType.MESH,
        )

    for k in order:
        tell(k).start()
    for k in order:
        if k not in early:
            inward(k, 0).start()
    for h in range(1, HALVES):
        for k in order:
            inward(k, h).start()
    for copy in own_in:
        copy.start()
    for k in order:
        tell(k).wait()

    n = members * parts
    mixed = pred[...].reshape(n, wide)
    spot = iota((n, n), 0)
    source = flip(me, spot // members, parts) * members + spot % members
    back = (iota((n, n), 1) == source).astype(F32)
    predicted = nn(back, mixed)
    here = ((targets >= 0) & (targets < tile_blocks)).astype(F32)
    mean = jnp.mean(predicted, axis=0, keepdims=True)
    scale = math.sqrt(float(PASS_COUNT)) * sigma[...]
    centred = (predicted - mean) / scale * here
    gap = jnp.broadcast_to((meas[...] - mean) / scale * here, predicted.shape)
    stats[0] = nt(centred, jnp.concatenate([centred, gap, draws[0], draws[1]], axis=0))

    def share(q):
        return pltpu.make_async_remote_copy(
            src_ref=stats.at[0], dst_ref=stats.at[q],
            send_sem=stat_send.at[q], recv_sem=stat_recv.at[q],
            device_id={"mem": me, "pix": flip(tile, q, tiles)}, device_id_type=pl.DeviceIdType.MESH,
        )

    for q in range(1, tiles):
        share(q).start()
    for q in range(1, tiles):
        share(q).wait()
    level = [stats[q] for q in range(tiles)]
    while len(level) > 1:
        level = [level[i] + level[i + 1] for i in range(0, len(level), 2)]
    expand(fold(level[0]), me, parts, times, mix)

    piece = math.gcd(half, 1024)
    own_out = []
    for h in range(HALVES):
        for k in order:
            inward(k, h).wait()
        own_in[h].wait()
        for k in order + [0]:
            for j in range(half // piece):
                at = slice(h * half + j * piece, h * half + (j + 1) * piece)
                both = jnp.dot(mix[k], held[:, at], preferred_element_type=F32)
                before = held[k * rows : (k + 1) * rows, at].astype(F32)
                fresh[k, :, at] = (before + both[:rows] + both[rows:]).astype(BF16)
            if k:
                outward(k, h).start()
            else:
                own_out.append(pltpu.make_async_copy(fresh.at[0, :, pl.ds(h * half, half)], out.at[:, columns(me, h)], own_sem.at[h]))
                own_out[-1].start()
    for h in range(HALVES):
        for k in order:
            outward(k, h).wait()
        own_out[h].wait()


def smoother(parts, tiles, prior, measured, noise, jitter, couples, target):
    members, times, cells = prior.shape
    rows = members * times
    width = cells // parts
    total = members * parts
    wide = -(-target.shape[1] // 128) * 128
    span = math.gcd(cells, 4096)
    dma = pltpu.SemaphoreType.DMA
    return pl.pallas_call(
        functools.partial(smoother_kernel, parts, tiles, times),
        in_specs=[pl.BlockSpec(memory_space=pl.ANY)] + [pl.BlockSpec(memory_space=pltpu.VMEM)] * 5,
        out_specs=pl.BlockSpec(memory_space=pl.ANY),
        out_shape=jax.ShapeDtypeStruct((rows, cells), BF16),
        scratch_shapes=[
            pltpu.VMEM((parts * rows, width), BF16),
            pltpu.VMEM((parts, rows, width), BF16),
            pltpu.VMEM((parts, 2 * rows, parts * rows), BF16),
            pltpu.VMEM((2, rows, span), BF16),
            pltpu.VMEM((rows, wide), F32),
            pltpu.VMEM((parts, members, wide), F32),
            pltpu.VMEM((tiles, total, 4 * total), F32),
            pltpu.VMEM((1, wide), jnp.int32),
            pltpu.VMEM((2, wide), jnp.int32),
            pltpu.VMEM((1, wide), F32),
            pltpu.VMEM((1, wide), F32),
            pltpu.VMEM((2, total, wide), F32),
            dma((parts, HALVES)), dma((parts, HALVES)), dma((parts, HALVES)), dma((parts, HALVES)),
            dma((parts,)), dma((parts,)), dma((tiles,)), dma((tiles,)),
            dma((2,)), dma((HALVES,)),
        ],
        compiler_params=pltpu.CompilerParams(
            collective_id=0, has_side_effects=True, vmem_limit_bytes=60 * 1024 * 1024
        ),
        name="smoother",
    )(prior.reshape(rows, cells), measured, noise, jitter, couples, target)


def solution(mesh):
    parts, tiles = mesh.shape["mem"], mesh.shape["pix"]

    def body(prior, measured, noise, jitter, couples, target):
        out = smoother(
            parts, tiles, prior, measured[None, :], noise[None, :],
            jnp.swapaxes(jitter, 1, 2), couples, target[None, :],
        )
        return out.reshape(prior.shape)

    return jax.shard_map(
        body,
        mesh=mesh,
        in_specs=(P("mem", None, "pix"), P(), P(), P(), P(), P()),
        out_specs=P("mem", None, "pix"),
        check_vma=False,
    )
```
